32 devices in a mesh: grp: 4 (over y, x), own: 8 (over z, core).
Axes of the slice: x: 2, y: 2, z: 4, core: 2. Of those that a mesh axis runs over, the one named last changes fastest.
Arguments:
- grad_parts: float32 [4, 8, 4, 8, 16, 2, 128], P('grp', 'own'), may hold values from -6 to 6
- block_ids: int32 [8, 4, 8, 16], P('own'), may hold values from 0 to 8191, as said below
- block_counts: int32 [8, 4, 8], P('own'), may hold values from 0 to 16, as said below
- params: float32 [8, 32768, 2, 128], P(None, ('grp', 'own')), may hold values from -4 to 4
- first_moment: float32 [8, 32768, 2, 128], P(None, ('grp', 'own')), may hold values from -2 to 2
- second_moment: float32 [8, 32768, 2, 128], P(None, ('grp', 'own')), may hold values from 0.0001 to 0.03
Outputs:
- new_params: float32 [8, 32768, 2, 128], P(None, ('grp', 'own'))
- new_first: float32 [8, 32768, 2, 128], P(None, ('grp', 'own'))
- new_second: float32 [8, 32768, 2, 128], P(None, ('grp', 'own'))
The draws below stay inside these ranges and needn't reach their ends.
Inputs may be any that keep to these rules, and one draw needn't show every extreme that they name: `block_ids`: within one row (fixed group and destination) the 16 block numbers are distinct; numbers in slots beyond the count are arbitrary but in range. `block_counts`: some destination device gets 16 used slots from every ray group.
All inputs are finite; a program needn't handle non-finite values.
Results may differ from the reference program's by a relative error of at most 0.00002.
Values sent between devices are 32-bit elements; how exact they have to be, the bound alone decides.
A program may use at most 128 MiB of HBM per device.

```python
import math
import jax
import jax.numpy as jnp
from jax import lax

LEVELS = 8
ENTRIES = 4194304
FEATURES = 2
BLOCK = 128
SLOTS = 16
NBLK = 32768
N_GRP = 4
N_OWN = 8
DEVICES = 32


def device_ramp(top):
    position = jnp.arange(N_GRP, dtype=jnp.float32)[:, None] * N_OWN + jnp.arange(N_OWN, dtype=jnp.float32)[None, :]
    level = jnp.exp(jnp.log(top) * position / (N_GRP * N_OWN - 1))
    return level.reshape(1, 1, N_GRP, N_OWN, 1, 1, 1)


def draw_grad_parts(key, part):
    shape = (N_GRP, N_OWN, N_GRP, N_OWN, SLOTS, FEATURES, BLOCK)
    ramp = device_ramp(8.0)
    values = 0.5 * ramp * jax.random.normal(jax.random.fold_in(key, 41), shape, dtype=jnp.float32)
    return jnp.clip(values, -6.0, 6.0).astype(jnp.float32)


def draw_block_ids(key, part):
    total = LEVELS * (ENTRIES // BLOCK // DEVICES)
    count_rows = N_OWN * N_GRP * N_OWN
    limit = 2 ** 31 // total - 1
    scores = jax.random.randint(jax.random.fold_in(key, 11), (count_rows, total), 0, limit, dtype=jnp.int32)
    scores = scores * total + jnp.arange(total, dtype=jnp.int32)[None, :]
    values, picked = lax.top_k(scores, SLOTS)
    return picked.astype(jnp.int32).reshape(N_OWN, N_GRP, N_OWN, SLOTS)


def draw_block_counts(key, part):
    first, second, third = jax.random.split(jax.random.fold_in(key, 23), 3)
    counts = jax.random.randint(first, (N_OWN, N_GRP, N_OWN), 0, SLOTS + 1, dtype=jnp.int32)
    row_grp = jax.random.randint(second, (), 0, N_GRP, dtype=jnp.int32)
    row_own = jax.random.randint(third, (), 0, N_OWN, dtype=jnp.int32)
    return counts.at[:, row_grp, row_own].set(SLOTS)


def levels(own_key, shape, shards, smallest, high):
    level = 1.0
    for dim, blocks in shards:
        draws = jax.random.uniform(jax.random.fold_in(jax.random.fold_in(own_key, 6), dim), (blocks,), jnp.float32, smallest / len(shards), high / len(shards))
        level = level * jnp.repeat(jnp.exp(draws), shape[dim] // blocks).reshape((-1,) + (1,) * (len(shape) - 1 - dim))
    return level


def gaussian(own_key, extent, scale, most, shards=(), kind=jnp.bfloat16):
    factor_of = levels(own_key, extent, shards, -0.22, 0.18) if shards else 1.0
    array = jax.random.normal(own_key, extent, jnp.float32) * scale * factor_of
    return jnp.minimum(jnp.maximum(array, -most), most).astype(kind)


def setup_inputs(seed: int = 0) -> dict:
    keys = jax.random.split(jax.random.key(seed), 7)
    return {
        "grad_parts": draw_grad_parts(jax.random.fold_in(keys[6], 71), 0),
        "block_ids": draw_block_ids(jax.random.fold_in(keys[6], 71), 0),
        "block_counts": draw_block_counts(jax.random.fold_in(keys[6], 71), 0),
        "params": gaussian(keys[3], (LEVELS, NBLK, FEATURES, BLOCK), 0.5, 4.0, ((1, 32),), jnp.float32),
        "first_moment": gaussian(keys[4], (LEVELS, NBLK, FEATURES, BLOCK), 0.3, 2.0, ((1, 32),), jnp.float32),
        "second_moment": jnp.clip(jnp.exp(math.log(0.03) - 5.7037825 * jax.random.uniform(keys[5], (LEVELS, NBLK, FEATURES, BLOCK), jnp.float32) ** levels(keys[5], (LEVELS, NBLK, FEATURES, BLOCK), ((1, 32),), -0.2, 0.2)), 0.0001, 0.03),
    }


def reference(grad_parts, block_ids, block_counts, params, first_moment, second_moment):
    blocks_level = ENTRIES // BLOCK
    per_device = blocks_level // DEVICES
    summed = lax.optimization_barrier(jnp.sum(grad_parts, axis=0))
    dest = jnp.arange(N_GRP, dtype=jnp.int32)[:, None] * N_OWN + jnp.arange(N_OWN, dtype=jnp.int32)[None, :]
    level = block_ids // per_device
    within = block_ids % per_device
    target = (level * blocks_level + dest[None, :, :, None] * per_device + within).astype(jnp.int32)
    valid = jnp.arange(SLOTS, dtype=jnp.int32)[None, None, None, :] < block_counts[..., None]
    width = FEATURES * BLOCK
    rows = summed.reshape(-1, width) * valid.reshape(-1, 1).astype(jnp.float32)
    segments = LEVELS * blocks_level
    dense = jax.ops.segment_sum(rows, target.reshape(-1), num_segments=segments)
    hits = jax.ops.segment_sum(valid.reshape(-1).astype(jnp.int32), target.reshape(-1), num_segments=segments) > 0
    square = jnp.sum(dense * dense)
    count = jnp.sum(hits.astype(jnp.float32))
    rms = jnp.sqrt(square / (count * width) + 1e-06)
    scale = jnp.minimum(jnp.float32(1.0), 0.5 / rms)
    clipped = scale * dense
    old_p = params.reshape(segments, width)
    old_m = first_moment.reshape(segments, width)
    old_v = second_moment.reshape(segments, width)
    mask = hits[:, None]
    new_m = jnp.where(mask, 0.9 * old_m + 0.1 * clipped, old_m)
    new_v = jnp.where(mask, 0.99 * old_v + 0.01 * clipped * clipped, old_v)
    stepped = old_p - 0.01 * (new_m / (1.0 - 0.9 ** 8)) / (jnp.sqrt(new_v / (1.0 - 0.99 ** 8)) + 1e-08)
    new_p = jnp.where(mask, stepped, old_p)
    shape = params.shape
    return (new_p.reshape(shape), new_m.reshape(shape), new_v.reshape(shape))
```

```python
import functools

import jax
import jax.numpy as jnp
from jax import lax
from jax.experimental import pallas as pl
from jax.experimental.pallas import tpu as pltpu
from jax.sharding import PartitionSpec as P

MESH = pl.DeviceIdType.MESH
HIGHEST = lax.Precision.HIGHEST
LANES = 128
PIECES = 4
ONE_M = 1.0 - 0.9**8
ONE_V = 1.0 - 0.99**8


def loop(count, body):
    if count <= 8:
        for i in range(count):
            body(i)
    else:

        def step(i, carry):
            body(i)
            return carry

        lax.fori_loop(0, count, step, 0)


def offset_of(i, n):
    return (n // 2 + ((i + 1) // 2) * (2 * (i % 2) - 1) + n) % n


def exchange_kernel(
    n_grp,
    n_own,
    slots,
    feats,
    grads,
    ids,
    counts,
    clip_out,
    keys_out,
    own_parts,
    got_parts,
    share,
    summed,
    key_send,
    key_got,
    dense,
    stat_send,
    stat_got,
    load_sem,
    part_send_sem,
    part_got_sem,
    share_send_sem,
    share_got_sem,
    key_send_sem,
    key_got_sem,
    stat_send_sem,
    stat_got_sem,
):
    my_g, my_o = lax.axis_index("grp"), lax.axis_index("own")
    n_dev = n_grp * n_own
    me = my_g * n_own + my_o
    per = slots * feats
    rows = n_own * per

    load = pltpu.make_async_copy(grads, own_parts, load_sem)
    load.start()
    barrier = pltpu.get_barrier_semaphore()

    def greet(i, carry):
        other = (me + 1 + i) % n_dev
        pl.semaphore_signal(
            barrier,
            inc=1,
            device_id={"grp": other // n_own, "own": other % n_own},
            device_id_type=MESH,
        )
        return carry

    lax.fori_loop(0, n_dev - 1, greet, 0)

    listing = ids[0, my_g].astype(jnp.float32)
    lane = lax.broadcasted_iota(jnp.int32, (slots, rows), 1)
    slot = lax.broadcasted_iota(jnp.int32, (slots, rows), 0)
    spread = jnp.where((lane % per) // feats == slot, 1.0, 0.0)
    wide = jnp.dot(listing, spread, precision=HIGHEST, preferred_element_type=jnp.float32)
    tally = counts[0, pl.ds(my_g, 1)].astype(jnp.float32)
    eye_r = lax.broadcasted_iota(jnp.int32, (n_own, n_own), 0)
    eye_c = lax.broadcasted_iota(jnp.int32, (n_own, n_own), 1)
    used = jnp.sum(jnp.where(eye_r == eye_c, jnp.broadcast_to(tally, (n_own, n_own)), 0.0), axis=1, keepdims=True)
    lane = lax.broadcasted_iota(jnp.int32, (n_own, rows), 1)
    number = ((lane % per) // feats).astype(jnp.float32)
    feature = (lane % feats).astype(jnp.float32)
    wide = jnp.where(number < used, jnp.round(wide) * feats + feature, -1.0)
    for o in range(n_own):
        key_send[o] = wide[o : o + 1]

    pl.semaphore_wait(barrier, n_dev - 1)

    def part_copy(i, hop):
        dest = (my_o + offset_of(i, n_own)) % n_own
        other = (my_g + hop + 1) % n_grp
        return pltpu.make_async_remote_copy(
            src_ref=own_parts.at[other, dest],
            dst_ref=got_parts.at[hop, dest],
            send_sem=part_send_sem.at[hop, i],
            recv_sem=part_got_sem.at[hop, i],
            device_id={"grp": other, "own": my_o},
            device_id_type=MESH,
        )

    def share_copy(i):
        dest = (my_o + offset_of(i, n_own)) % n_own
        return pltpu.make_async_remote_copy(
            src_ref=share.at[dest],
            dst_ref=summed.at[my_o],
            send_sem=share_send_sem.at[i],
            recv_sem=share_got_sem.at[i],
            device_id={"grp": my_g, "own": dest},
            device_id_type=MESH,
        )

    def key_copy(i):
        dest = (my_o + offset_of(i, n_own)) % n_own
        return pltpu.make_async_remote_copy(
            src_ref=key_send.at[dest],
            dst_ref=key_got.at[my_o],
            send_sem=key_send_sem.at[i],
            recv_sem=key_got_sem.at[i],
            device_id={"grp": my_g, "own": dest},
            device_id_type=MESH,
        )

    def stat_copy(i):
        other = (me + 1 + i) % n_dev
        return pltpu.make_async_remote_copy(
            src_ref=stat_send,
            dst_ref=stat_got.at[me],
            send_sem=stat_send_sem.at[i],
            recv_sem=stat_got_sem.at[i],
            device_id={"grp": other // n_own, "own": other % n_own},
            device_id_type=MESH,
        )

    load.wait()

    def send_parts(i):
        for hop in range(n_grp - 1):
            part_copy(i, hop).start()

    loop(n_own, send_parts)
    loop(n_own - 1, lambda i: key_copy(i).start())
    key_got[my_o] = key_send[my_o]

    def total_of(i):
        dest = (my_o + offset_of(i, n_own)) % n_own
        for hop in range(n_grp - 1):
            part_copy(i, hop).wait_recv()
        total = own_parts[my_g, dest]
        for hop in range(n_grp - 1):
            total = total + got_parts[hop, dest]
        return total

    def forward(i):
        dest = (my_o + offset_of(i, n_own)) % n_own
        share[dest] = total_of(i)
        share_copy(i).start()

    loop(n_own - 1, forward)
    summed[my_o] = total_of(n_own - 1)

    loop(n_own - 1, lambda i: key_copy(i).wait_recv())
    lane = lax.broadcasted_iota(jnp.int32, (n_own, rows), 1)
    source = lax.broadcasted_iota(jnp.int32, (n_own, rows), 0)
    keys = jnp.sum(jnp.where(lane // per == source, key_got[...].reshape(n_own, rows), 0.0), axis=0, keepdims=True)
    keys_out[...] = keys.astype(jnp.int32)
    tile = 256
    equals = []
    earlier = jnp.zeros((1, rows), jnp.float32)
    for b in range(rows // tile):
        column = jnp.transpose(jnp.broadcast_to(keys[:, b * tile : (b + 1) * tile], (LANES, tile)))
        column = jnp.concatenate([column] * (rows // LANES), axis=1)
        equal = jnp.where((column == keys) & (keys >= 0.0), 1.0, 0.0)
        down = lax.broadcasted_iota(jnp.int32, (tile, rows), 0) + b * tile
        right = lax.broadcasted_iota(jnp.int32, (tile, rows), 1)
        earlier = earlier + jnp.sum(jnp.where(down < right, equal, 0.0), axis=0, keepdims=True)
        equals.append(equal)
    first = jnp.where((earlier == 0.0) & (keys >= 0.0), 1.0, 0.0)

    loop(n_own - 1, lambda i: share_copy(i).wait_recv())
    slots_in = summed[...].reshape(rows, LANES)
    for b in range(rows // tile):
        dense[b * tile : (b + 1) * tile] = jnp.dot(
            equals[b], slots_in, precision=HIGHEST, preferred_element_type=jnp.float32
        )
    whole = dense[...]
    squares = jnp.dot(
        jnp.broadcast_to(first, (8, rows)), whole * whole, precision=HIGHEST, preferred_element_type=jnp.float32
    )
    square = jnp.sum(squares[0:1], axis=1, keepdims=True)
    touched = jnp.sum(first, axis=1, keepdims=True)
    spot = lax.broadcasted_iota(jnp.int32, (1, LANES), 1)
    stat = jnp.where(spot == 0, square, jnp.where(spot == 1, touched, 0.0))
    stat_send[...] = stat
    stat_got[me] = stat

    def send_stat(i, carry):
        stat_copy(i).start()
        return carry

    lax.fori_loop(0, n_dev - 1, send_stat, 0)

    def end_parts(i):
        for hop in range(n_grp - 1):
            part_copy(i, hop).wait_send()

    loop(n_own, end_parts)
    loop(n_own - 1, lambda i: key_copy(i).wait_send())
    loop(n_own - 1, lambda i: share_copy(i).wait_send())

    def get_stat(i, carry):
        stat_copy(i).wait_recv()
        return carry

    lax.fori_loop(0, n_dev - 1, get_stat, 0)
    stats = jnp.sum(stat_got[...].reshape(n_dev, LANES), axis=0, keepdims=True)
    square = jnp.sum(jnp.where(spot == 0, stats, 0.0), axis=1, keepdims=True)
    touched = jnp.sum(jnp.where(spot == 1, stats, 0.0), axis=1, keepdims=True)
    rms = jnp.sqrt(square / (touched * LANES) + 1e-06)
    scale = jnp.minimum(1.0, 0.5 / rms)
    clip_out[...] = scale * dense[...]

    def end_stat(i, carry):
        stat_copy(i).wait_send()
        return carry

    lax.fori_loop(0, n_dev - 1, end_stat, 0)


def update_kernel(
    feats, keys, clipped, old_p, old_m, old_v, new_p, new_m, new_v, p, m, v, rows_p, rows_m, rows_v, in_sem, out_sem
):
    total = p.shape[0]
    piece = total // PIECES
    trio = ((old_p, p, new_p), (old_m, m, new_m), (old_v, v, new_v))
    reads = []
    for a, (old, held, _) in enumerate(trio):
        for q in range(PIECES):
            part = pl.ds(q * piece, piece)
            reads.append(pltpu.make_async_copy(old.at[part], held.at[part], in_sem.at[a, q]))
    for read in reads:
        read.start()
    for read in reads:
        read.wait()
    count = clipped.shape[0] // feats

    def gather(t, carry):
        block = jnp.maximum(keys[0, t * feats], 0) // feats
        spot = pl.ds(t * feats, feats)
        rows_p[spot] = p[block]
        rows_m[spot] = m[block]
        rows_v[spot] = v[block]
        return carry

    lax.fori_loop(0, count, gather, 0, unroll=16)
    c = clipped[...]
    fresh_m = 0.9 * rows_m[...] + 0.1 * c
    fresh_v = 0.99 * rows_v[...] + 0.01 * c * c
    rows_p[...] = rows_p[...] - 0.01 * (fresh_m / ONE_M) / (jnp.sqrt(fresh_v / ONE_V) + 1e-08)
    rows_m[...] = fresh_m
    rows_v[...] = fresh_v

    writes = []
    for a, ((_, held, new), fresh) in enumerate(zip(trio, (rows_p, rows_m, rows_v))):

        def scatter(t, carry):
            key = keys[0, t * feats]

            @pl.when(key >= 0)
            def _():
                held[key // feats] = fresh[pl.ds(t * feats, feats)]

            return carry

        lax.fori_loop(0, count, scatter, 0, unroll=16)
        for q in range(PIECES):
            part = pl.ds(q * piece, piece)
            write = pltpu.make_async_copy(held.at[part], new.at[part], out_sem.at[a, q])
            write.start()
            writes.append(write)
    for write in writes:
        write.wait()


def shards(n_grp, n_own, grad_parts, block_ids, block_counts, params, first_moment, second_moment):
    slots, feats, width = grad_parts.shape[4:]
    per = slots * feats
    rows = n_own * per
    n_dev = n_grp * n_own
    f32 = jnp.float32
    vmem = pl.BlockSpec(memory_space=pltpu.VMEM)
    hbm = pl.BlockSpec(memory_space=pl.ANY)
    dma = pltpu.SemaphoreType.DMA
    clipped, keys = pl.pallas_call(
        functools.partial(exchange_kernel, n_grp, n_own, slots, feats),
        out_shape=(jax.ShapeDtypeStruct((rows, width), f32), jax.ShapeDtypeStruct((1, rows), jnp.int32)),
        in_specs=[hbm, vmem, vmem],
        out_specs=(vmem, vmem),
        scratch_shapes=[
            pltpu.VMEM((n_grp, n_own, per, width), f32),
            pltpu.VMEM((n_grp - 1, n_own, per, width), f32),
            pltpu.VMEM((n_own, per, width), f32),
            pltpu.VMEM((n_own, per, width), f32),
            pltpu.VMEM((n_own, 1, rows), f32),
            pltpu.VMEM((n_own, 1, rows), f32),
            pltpu.VMEM((rows, width), f32),
            pltpu.VMEM((1, LANES), f32),
            pltpu.VMEM((n_dev, 1, LANES), f32),
            dma,
            dma((n_grp - 1, n_own)),
            dma((n_grp - 1, n_own)),
            dma((n_own,)),
            dma((n_own,)),
            dma((n_own,)),
            dma((n_own,)),
            dma((n_dev,)),
            dma((n_dev,)),
        ],
        compiler_params=pltpu.CompilerParams(collective_id=0, has_side_effects=True),
        name="exchange",
    )(grad_parts.reshape(n_grp, n_own, per, width), block_ids, block_counts)

    shape = params.shape
    blocks = shape[0] * shape[1]
    table = jax.ShapeDtypeStruct((blocks, feats, width), f32)
    outs = pl.pallas_call(
        functools.partial(update_kernel, feats),
        out_shape=(table,) * 3,
        in_specs=[pl.BlockSpec(memory_space=pltpu.SMEM), vmem, hbm, hbm, hbm],
        out_specs=(hbm,) * 3,
        scratch_shapes=[pltpu.VMEM((blocks, feats, width), f32)] * 3
        + [pltpu.VMEM((rows, width), f32)] * 3
        + [dma((3, PIECES))] * 2,
        name="update",
    )(keys, clipped, *(x.reshape(blocks, feats, width) for x in (params, first_moment, second_moment)))
    return tuple(x.reshape(shape) for x in outs)


def solution(mesh):
    n_grp, n_own = mesh.shape["grp"], mesh.shape["own"]
    table = P(None, ("grp", "own"), None, None)
    return jax.shard_map(
        functools.partial(shards, n_grp, n_own),
        mesh=mesh,
        in_specs=(
            P("grp", "own", None, None, None, None, None),
            P("own", None, None, None),
            P("own", None, None),
            table,
            table,
            table,
        ),
        out_specs=(table, table, table),
        check_vma=False,
    )
```

```python
import functools

import jax
import jax.numpy as jnp
from jax import lax
from jax.experimental import pallas as pl
from jax.experimental.pallas import tpu as pltpu
from jax.sharding import PartitionSpec as P

MESH = pl.DeviceIdType.MESH
HIGHEST = lax.Precision.HIGHEST
LANES = 128
PIECES = 4
EXCHANGE_VMEM = 32 << 20
WRITE_VMEM = 2 << 20
ONE_M = 1.0 - 0.9**8
ONE_V = 1.0 - 0.99**8


def loop(count, body):
    if count <= 8:
        for i in range(count):
            body(i)
    else:

        def step(i, carry):
            body(i)
            return carry

        lax.fori_loop(0, count, step, 0)


def offset_of(i, n):
    return (n // 2 + ((i + 1) // 2) * (2 * (i % 2) - 1) + n) % n


def exchange_kernel(
    n_grp,
    n_own,
    slots,
    feats,
    grads,
    ids,
    counts,
    old_p,
    old_m,
    old_v,
    keys_out,
    rows_p,
    rows_m,
    rows_v,
    held_p,
    held_m,
    held_v,
    own_parts,
    got_parts,
    share,
    summed,
    key_send,
    key_got,
    dense,
    stat_send,
    stat_got,
    key_scalars,
    load_sem,
    table_sem,
    scalar_sem,
    part_send_sem,
    part_got_sem,
    share_send_sem,
    share_got_sem,
    key_send_sem,
    key_got_sem,
    stat_send_sem,
    stat_got_sem,
):
    my_g, my_o = lax.axis_index("grp"), lax.axis_index("own")
    n_dev = n_grp * n_own
    me = my_g * n_own + my_o
    per = slots * feats
    rows = n_own * per

    load = pltpu.make_async_copy(grads, own_parts, load_sem)
    load.start()
    piece = old_p.shape[0] // PIECES
    reads = []
    for a, (old, held) in enumerate(((old_p, held_p), (old_m, held_m), (old_v, held_v))):
        for q in range(PIECES):
            part = pl.ds(q * piece, piece)
            reads.append(pltpu.make_async_copy(old.at[part], held.at[part], table_sem.at[a, q]))
    barrier = pltpu.get_barrier_semaphore()

    def greet(i, carry):
        other = (me + 1 + i) % n_dev
        pl.semaphore_signal(
            barrier,
            inc=1,
            device_id={"grp": other // n_own, "own": other % n_own},
            device_id_type=MESH,
        )
        return carry

    lax.fori_loop(0, n_dev - 1, greet, 0)

    listing = ids[0, my_g]
    lane = lax.broadcasted_iota(jnp.int32, (n_own, rows), 1)
    number = (lane % per) // feats
    wide = jnp.broadcast_to(listing[:, 0:1], (n_own, rows))
    for j in range(1, slots):
        wide = jnp.where(number == j, listing[:, j : j + 1], wide)
    tally = counts[0, pl.ds(my_g, 1)]
    eye_r = lax.broadcasted_iota(jnp.int32, (n_own, n_own), 0)
    eye_c = lax.broadcasted_iota(jnp.int32, (n_own, n_own), 1)
    used = jnp.sum(jnp.where(eye_r == eye_c, jnp.broadcast_to(tally, (n_own, n_own)), 0), axis=1, keepdims=True)
    wide = jnp.where(number < used, wide * feats + lane % feats, -1)
    for o in range(n_own):
        key_send[o] = wide[o : o + 1]

    pl.semaphore_wait(barrier, n_dev - 1)

    def part_copy(i, hop):
        dest = (my_o + offset_of(i, n_own)) % n_own
        other = (my_g + hop + 1) % n_grp
        return pltpu.make_async_remote_copy(
            src_ref=own_parts.at[other, dest],
            dst_ref=got_parts.at[hop, dest],
            send_sem=part_send_sem.at[hop, i],
            recv_sem=part_got_sem.at[hop, i],
            device_id={"grp": other, "own": my_o},
            device_id_type=MESH,
        )

    def share_copy(i):
        dest = (my_o + offset_of(i, n_own)) % n_own
        return pltpu.make_async_remote_copy(
            src_ref=share.at[dest],
            dst_ref=summed.at[my_o],
            send_sem=share_send_sem.at[i],
            recv_sem=share_got_sem.at[i],
            device_id={"grp": my_g, "own": dest},
            device_id_type=MESH,
        )

    def key_copy(i):
        dest = (my_o + offset_of(i, n_own)) % n_own
        return pltpu.make_async_remote_copy(
            src_ref=key_send.at[dest],
            dst_ref=key_got.at[my_o],
            send_sem=key_send_sem.at[i],
            recv_sem=key_got_sem.at[i],
            device_id={"grp": my_g, "own": dest},
            device_id_type=MESH,
        )

    def stat_copy(i):
        other = (me + 1 + i) % n_dev
        return pltpu.make_async_remote_copy(
            src_ref=stat_send,
            dst_ref=stat_got.at[me],
            send_sem=stat_send_sem.at[i],
            recv_sem=stat_got_sem.at[i],
            device_id={"grp": other // n_own, "own": other % n_own},
            device_id_type=MESH,
        )

    load.wait()
    for read in reads:
        read.start()

    def send_parts(i):
        for hop in range(n_grp - 1):
            part_copy(i, hop).start()

    loop(n_own, send_parts)
    loop(n_own - 1, lambda i: key_copy(i).start())
    key_got[my_o] = key_send[my_o]

    def total_of(i):
        dest = (my_o + offset_of(i, n_own)) % n_own
        for hop in range(n_grp - 1):
            part_copy(i, hop).wait_recv()
        total = own_parts[my_g, dest]
        for hop in range(n_grp - 1):
            total = total + got_parts[hop, dest]
        return total

    def forward(i):
        dest = (my_o + offset_of(i, n_own)) % n_own
        share[dest] = total_of(i)
        share_copy(i).start()

    loop(n_own - 1, forward)
    summed[my_o] = total_of(n_own - 1)

    loop(n_own - 1, lambda i: key_copy(i).wait_recv())
    lane = lax.broadcasted_iota(jnp.int32, (n_own, rows), 1)
    source = lax.broadcasted_iota(jnp.int32, (n_own, rows), 0)
    keys = jnp.sum(jnp.where(lane // per == source, key_got[...].reshape(n_own, rows), 0), axis=0, keepdims=True)
    keys_out[...] = keys
    to_scalars = pltpu.make_async_copy(keys_out, key_scalars, scalar_sem)
    to_scalars.start()
    tile = 256
    equals = []
    earlier = jnp.zeros((1, rows), jnp.float32)
    for b in range(rows // tile):
        column = jnp.transpose(jnp.broadcast_to(keys[:, b * tile : (b + 1) * tile], (LANES, tile)))
        column = jnp.concatenate([column] * (rows // LANES), axis=1)
        equal = jnp.where((column == keys) & (keys >= 0), 1.0, 0.0)
        down = lax.broadcasted_iota(jnp.int32, (tile, rows), 0) + b * tile
        right = lax.broadcasted_iota(jnp.int32, (tile, rows), 1)
        earlier = earlier + jnp.sum(jnp.where(down < right, equal, 0.0), axis=0, keepdims=True)
        equals.append(equal)
    first = jnp.where((earlier == 0.0) & (keys >= 0), 1.0, 0.0)

    loop(n_own - 1, lambda i: share_copy(i).wait_recv())
    slots_in = summed[...].reshape(rows, LANES)
    for b in range(rows // tile):
        dense[b * tile : (b + 1) * tile] = jnp.dot(
            equals[b], slots_in, precision=HIGHEST, preferred_element_type=jnp.float32
        )
    whole = dense[...]
    squares = jnp.dot(
        jnp.broadcast_to(first, (8, rows)), whole * whole, precision=HIGHEST, preferred_element_type=jnp.float32
    )
    square = jnp.sum(squares[0:1], axis=1, keepdims=True)
    touched = jnp.sum(first, axis=1, keepdims=True)
    spot = lax.broadcasted_iota(jnp.int32, (1, LANES), 1)
    stat = jnp.where(spot == 0, square, jnp.where(spot == 1, touched, 0.0))
    stat_send[...] = stat
    stat_got[me] = stat

    def send_stat(i, carry):
        stat_copy(i).start()
        return carry

    lax.fori_loop(0, n_dev - 1, send_stat, 0)

    def end_parts(i):
        for hop in range(n_grp - 1):
            part_copy(i, hop).wait_send()

    loop(n_own, end_parts)
    loop(n_own - 1, lambda i: key_copy(i).wait_send())
    loop(n_own - 1, lambda i: share_copy(i).wait_send())

    to_scalars.wait()
    for read in reads:
        read.wait()

    def gather(t, carry):
        block = jnp.clip(key_scalars[0, t * feats] // feats, 0, held_p.shape[0] - 1)
        spot = pl.ds(t * feats, feats)
        rows_p[spot] = held_p[block]
        rows_m[spot] = held_m[block]
        rows_v[spot] = held_v[block]
        return carry

    lax.fori_loop(0, rows // feats, gather, 0, unroll=16)

    def get_stat(i, carry):
        stat_copy(i).wait_recv()
        return carry

    lax.fori_loop(0, n_dev - 1, get_stat, 0)
    stats = jnp.sum(stat_got[...].reshape(n_dev, LANES), axis=0, keepdims=True)
    square = jnp.sum(jnp.where(spot == 0, stats, 0.0), axis=1, keepdims=True)
    touched = jnp.sum(jnp.where(spot == 1, stats, 0.0), axis=1, keepdims=True)
    rms = jnp.sqrt(square / (touched * LANES) + 1e-06)
    scale = jnp.minimum(1.0, 0.5 / rms)
    clipped = scale * dense[...]
    fresh_m = 0.9 * rows_m[...] + 0.1 * clipped
    fresh_v = 0.99 * rows_v[...] + 0.01 * clipped * clipped
    rows_p[...] = rows_p[...] - 0.01 * (fresh_m / ONE_M) / (jnp.sqrt(fresh_v / ONE_V) + 1e-08)
    rows_m[...] = fresh_m
    rows_v[...] = fresh_v

    def end_stat(i, carry):
        stat_copy(i).wait_send()
        return carry

    lax.fori_loop(0, n_dev - 1, end_stat, 0)


def write_kernel(feats, keys, rows_p, rows_m, rows_v, old_p, old_m, old_v, p, m, v, new_p, new_m, new_v, sem):
    piece = p.shape[0] // PIECES
    count = rows_p.shape[0] // feats
    writes = []
    for a, (fresh, held, new) in enumerate(((rows_p, p, new_p), (rows_m, m, new_m), (rows_v, v, new_v))):

        def scatter(t, carry):
            key = keys[0, t * feats]

            @pl.when(key >= 0)
            def _():
                held[key // feats] = fresh[pl.ds(t * feats, feats)]

            return carry

        lax.fori_loop(0, count, scatter, 0, unroll=16)
        for q in range(PIECES):
            part = pl.ds(q * piece, piece)
            write = pltpu.make_async_copy(held.at[part], new.at[part], sem.at[a, q])
            write.start()
            writes.append(write)
    for write in writes:
        write.wait()


def shards(n_grp, n_own, grad_parts, block_ids, block_counts, params, first_moment, second_moment):
    slots, feats, width = grad_parts.shape[4:]
    per = slots * feats
    rows = n_own * per
    n_dev = n_grp * n_own
    f32 = jnp.float32
    vmem = pl.BlockSpec(memory_space=pltpu.VMEM)
    hbm = pl.BlockSpec(memory_space=pl.ANY)
    dma = pltpu.SemaphoreType.DMA
    shape = params.shape
    blocks = shape[0] * shape[1]
    table = (blocks, feats, width)
    keys, rows_p, rows_m, rows_v, *held = pl.pallas_call(
        functools.partial(exchange_kernel, n_grp, n_own, slots, feats),
        out_shape=(pltpu.VMEM((1, rows), jnp.int32),)
        + (pltpu.VMEM((rows, width), f32),) * 3
        + (pltpu.VMEM(table, f32),) * 3,
        in_specs=[hbm, vmem, vmem, hbm, hbm, hbm],
        out_specs=(vmem,) * 7,
        scratch_shapes=[
            pltpu.VMEM((n_grp, n_own, per, width), f32),
            pltpu.VMEM((n_grp - 1, n_own, per, width), f32),
            pltpu.VMEM((n_own, per, width), f32),
            pltpu.VMEM((n_own, per, width), f32),
            pltpu.VMEM((n_own, 1, rows), jnp.int32),
            pltpu.VMEM((n_own, 1, rows), jnp.int32),
            pltpu.VMEM((rows, width), f32),
            pltpu.VMEM((1, LANES), f32),
            pltpu.VMEM((n_dev, 1, LANES), f32),
            pltpu.SMEM((1, rows), jnp.int32),
            dma,
            dma((3, PIECES)),
            dma,
            dma((n_grp - 1, n_own)),
            dma((n_grp - 1, n_own)),
            dma((n_own,)),
            dma((n_own,)),
            dma((n_own,)),
            dma((n_own,)),
            dma((n_dev,)),
            dma((n_dev,)),
        ],
        compiler_params=pltpu.CompilerParams(
            collective_id=0, has_side_effects=True, vmem_limit_bytes=EXCHANGE_VMEM
        ),
        name="exchange",
    )(
        grad_parts.reshape(n_grp, n_own, per, width),
        block_ids,
        block_counts,
        *(pltpu.with_memory_space_constraint(x.reshape(table), pltpu.HBM) for x in (params, first_moment, second_moment)),
    )

    outs = pl.pallas_call(
        functools.partial(write_kernel, feats),
        out_shape=(pltpu.VMEM(table, f32),) * 3 + (jax.ShapeDtypeStruct(table, f32),) * 3,
        in_specs=[pl.BlockSpec(memory_space=pltpu.SMEM)] + [vmem] * 6,
        out_specs=(vmem,) * 3 + (pl.BlockSpec(memory_space=pltpu.HBM),) * 3,
        input_output_aliases={4: 0, 5: 1, 6: 2},
        scratch_shapes=[dma((3, PIECES))],
        compiler_params=pltpu.CompilerParams(vmem_limit_bytes=WRITE_VMEM),
        name="write",
    )(keys, rows_p, rows_m, rows_v, *held)
    return tuple(x.reshape(shape) for x in outs[3:])


def solution(mesh):
    n_grp, n_own = mesh.shape["grp"], mesh.shape["own"]
    table = P(None, ("grp", "own"), None, None)
    return jax.shard_map(
        functools.partial(shards, n_grp, n_own),
        mesh=mesh,
        in_specs=(
            P("grp", "own", None, None, None, None, None),
            P("own", None, None, None),
            P("own", None, None),
            table,
            table,
            table,
        ),
        out_specs=(table, table, table),
        check_vma=False,
    )
```
